32 devices in a mesh: expert: 8 (over z, y), vocab: 4 (over x, core).
Axes of the slice: x: 2, y: 2, z: 4, core: 2. Of those that a mesh axis runs over, the one named last changes fastest.
Arguments:
- tokens: bfloat16 [1024, 2048], P('expert'), may hold values from -12 to 12
- expert_ids: int32 [1024, 6], P('expert'), may hold values from 0 to 15, all different within a row; in each aligned block of 128 rows (0 to 127, 128 to 255, ...) at most 96 rows name the same one
- gates: float32 [1024, 6], P('expert'), may hold values from 0.05 to 0.4
- w_gate: bfloat16 [16, 2048, 1408], P('expert', None, 'vocab'), may hold values from -0.125 to 0.125
- w_up: bfloat16 [16, 2048, 1408], P('expert', None, 'vocab'), may hold values from -0.125 to 0.125
- w_down: bfloat16 [16, 1408, 2048], P('expert', 'vocab'), may hold values from -0.21875 to 0.21875
- norm_gain: float32 [2048], replicated, may hold values from 0.5 to 1.5
- lm_weight: bfloat16 [2048, 24576], P(None, ('expert', 'vocab')), may hold values from -6.9605824 to 6.9605824
- targets: int32 [1024], P('expert'), may hold values from 0 to 24575
Outputs:
- logprobs: float32 [1024], P('expert')
The draws below stay inside these ranges and needn't reach their ends.
Inputs may be any that keep to these rules, and one draw needn't show every extreme that they name: `expert_ids`: in the 128 rows of one device no expert is named by more than 96 routes; each row names 6 different experts.
All inputs are finite; a program needn't handle non-finite values.
Results may differ from the reference program's by a relative error of at most 0.003.
Values may be sent and summed in bfloat16 or wider, within the bound.
No kernel may reach another device: no remote copies, remote signals or barrier semaphores. Data moves between devices by JAX's collectives and lax.ppermute only.
A program may use at most 128 MiB of HBM per device.

```python
import math
import jax
import jax.numpy as jnp
import numpy as np
from jax import lax

D = 2048
FF = 1408
TOP = 6
TOK_DEV = 128
EXPERTS = 16
TOKENS = 1024
VOCAB = 24576
CAP = 96
N_EXPERT = 8


def draw_tokens(key, part):
    first_key = jax.random.fold_in(jax.random.fold_in(key, 11), 0)
    column = jnp.arange(D, dtype=jnp.float32)
    col_scale = 0.6 + 1.2 * column / D
    values = jnp.clip(jax.random.normal(first_key, (TOKENS, D), jnp.float32), -6.0, 6.0)
    return (values * col_scale[None, :]).astype(jnp.bfloat16)


def draw_lm_weight(key, part):
    inner_key = jax.random.fold_in(key, 23)
    values = jnp.clip(jax.random.normal(inner_key, (D, VOCAB), jnp.float32), -6.0, 6.0)
    return (values * 6.0 / jnp.sqrt(jnp.float32(D))).astype(jnp.bfloat16)


def plant(drawn, stream_key, least, largest):
    longest = drawn.shape.index(max(drawn.shape))
    spots = []
    for shift in (0, 1):
        where = [jax.random.randint(jax.random.fold_in(stream_key, axis), (), 0, length) for axis, length in enumerate(drawn.shape)]
        where[longest] = (where[longest] + shift) % drawn.shape[longest]
        spots.append(tuple(where))
    return drawn.at[spots[0]].set(least).at[spots[1]].set(largest)


def spiked(result, rng, source, target, parts, factor):
    owner, partner = [(jnp.arange(result.shape[dim]) // (result.shape[dim] // parts)).reshape([-1 if axis == dim else 1 for axis in range(result.ndim)]) for dim in (source, target)]
    chosen = jax.random.permutation(rng, parts)[partner]
    strong = (owner == chosen) | (owner == (partner + parts // 2) % parts)
    return jnp.where(strong, factor * result, result)


def shard_levels(rng, dims, cuts, smallest, largest):
    def one(dim, shards_of):
        steps = jax.random.uniform(jax.random.fold_in(jax.random.fold_in(rng, 6), dim), (shards_of,), jnp.float32, smallest / len(cuts), largest / len(cuts))
        return jnp.repeat(jnp.exp(steps), dims[dim] // shards_of).reshape((-1,) + (1,) * (len(dims) - dim - 1))

    loudness = one(*cuts[0])
    for cut in cuts[1:]:
        loudness = loudness * one(*cut)
    return loudness


def deal_out(key, own, number, rows, count, top, most, lean):
    order = jax.random.permutation(key, count)
    heavy_load, ordinary = shares(count, rows * top, most, lean, True), shares(count, rows * top, most, lean, False)
    places = jnp.arange(count)

    def named(lengths, rotation):
        used = int((lengths > 0).sum())
        fixed = max(1, used // 4)
        passed = fixed + (places - fixed + rotation * (used - fixed)) % max(1, count - fixed)
        return jnp.zeros((count,), jnp.int32).at[order[jnp.where(places < fixed, places, passed)]].set(jnp.asarray(lengths, jnp.int32))

    lengths = jnp.where(number % 4 == 0, named(heavy_load, number // 4), named(ordinary, number - number // 4 - 1))
    mixed = jax.random.permutation(jax.random.fold_in(own, 3), count)
    donor, receiver = mixed[0:count // 2 * 2:2], mixed[1:count // 2 * 2:2]
    slack = jnp.minimum(lengths[donor] - 1, most - lengths[receiver]) // 2
    slack = jnp.where((donor == order[0]) | (receiver == order[0]) | (lengths[receiver] == 0), 0, jnp.maximum(slack, 0))
    passed = jax.random.randint(jax.random.fold_in(own, 4), (count // 2,), 0, 1 << 20) % (slack + 1)
    lengths = lengths.at[donor].add(-passed).at[receiver].add(passed)
    members = jnp.searchsorted(jnp.cumsum(lengths), jnp.arange(rows * top), side="right").astype(jnp.int32)
    listing = members.reshape(top, rows).T
    listing = listing[jax.random.permutation(jax.random.fold_in(own, 1), rows)]
    rotation = jax.random.randint(jax.random.fold_in(own, 2), (rows, 1), 0, top)
    return jnp.take_along_axis(listing, (jnp.arange(top)[None, :] + rotation) % top, axis=1)


def shares(number_of, total, limit, skew, full):
    weights = [(1 << 20) // math.isqrt(grade ** skew) + 1 for grade in range(1, number_of + 1)]
    largest = limit if full else min(limit, max(-(-total // number_of), total * weights[0] // sum(weights)))
    least = 1 if total - largest >= number_of - 1 else 0
    counts, surplus = [largest] + [least] * (number_of - 1), total - largest - least * (number_of - 1)
    while surplus > 0:
        free = [i for i in range(1, number_of) if counts[i] < largest] or [i for i in range(1, number_of) if counts[i] < limit]
        whole, remaining = sum([weights[i] for i in free]), surplus
        for i in free:
            more = min(limit - counts[i], max(1, remaining * weights[i] // whole), surplus)
            counts[i] = counts[i] + more
            surplus = surplus - more
    return np.array(counts)


def scatter_about(stream_key, dims, scale, reach, shards=(), kind=jnp.bfloat16):
    loudness = shard_levels(stream_key, dims, shards, -0.22, 0.18) if shards else 1.0
    values = jax.random.normal(stream_key, dims, jnp.float32) * scale * loudness
    return jnp.minimum(jnp.maximum(values, -reach), reach).astype(kind)


def heavy_noise(key, extent, spread, reach, pieces, heavy, kind=jnp.bfloat16):
    array = spread * jax.random.normal(key, extent, jnp.float32)
    if pieces:
        array = array * shard_levels(key, extent, pieces, -0.22, 0.18)
    return jnp.clip(spiked(array, jax.random.fold_in(key, 3), *heavy), -reach, reach).astype(kind)


def setup_inputs(seed: int = 0) -> dict:
    keys = jax.random.split(jax.random.key(seed), 10)
    tokens = draw_tokens(jax.random.fold_in(keys[9], 71), 0)
    expert_ids_keys = jax.random.split(jax.random.fold_in(keys[1], 1), TOKENS // TOK_DEV)
    expert_ids_turns = jax.random.permutation(jax.random.fold_in(keys[1], 3), TOKENS // TOK_DEV)
    expert_ids = jax.vmap(lambda own, number: deal_out(jax.random.fold_in(keys[1], 2), own, number, TOK_DEV, EXPERTS, TOP, CAP, 2))(expert_ids_keys, expert_ids_turns).reshape((TOKENS, TOP))
    gates = jnp.clip(jnp.exp(math.log(0.4) - 2.0794415 * jax.random.uniform(keys[2], (TOKENS, TOP), jnp.float32) ** shard_levels(keys[2], (TOKENS, TOP), ((0, 8),), -0.2, 0.2)), 0.05, 0.4)
    w_gate = scatter_about(keys[3], (EXPERTS, D, FF), D ** -0.5, 0.125, ((0, 8), (2, 4)))
    w_up = scatter_about(keys[4], (EXPERTS, D, FF), D ** -0.5, 0.125, ((0, 8), (2, 4)))
    w_down = heavy_noise(keys[5], (EXPERTS, FF, D), FF ** -0.5, 0.21875, ((0, 8), (1, 4)), (1, 2, 4, 2.0))
    norm_gain = jnp.clip(1.0 + 0.1 * jax.random.normal(keys[6], (D,), jnp.float32), 0.5, 1.5)
    lm_weight = draw_lm_weight(jax.random.fold_in(keys[9], 71), 0)
    targets = plant(jax.random.randint(keys[8], (TOKENS,), 0, VOCAB), jax.random.fold_in(keys[8], 1), 0, VOCAB - 1).astype(jnp.int32)
    return {"tokens": tokens, "expert_ids": expert_ids, "gates": gates, "w_gate": w_gate, "w_up": w_up, "w_down": w_down, "norm_gain": norm_gain, "lm_weight": lm_weight, "targets": targets}


def expert_ffn(rows, gate_mat, up_mat, down_mat):
    gate_val = jnp.dot(rows, gate_mat, preferred_element_type=jnp.float32)
    up_val = jnp.dot(rows, up_mat, preferred_element_type=jnp.float32)
    hidden = (jax.nn.silu(gate_val) * up_val).astype(jnp.bfloat16)
    return jnp.dot(hidden, down_mat, preferred_element_type=jnp.float32)

def reference(tokens, expert_ids, gates, w_gate, w_up, w_down, norm_gain, lm_weight, targets):
    sources = N_EXPERT
    block_ids = expert_ids.reshape(sources, TOK_DEV * TOP).astype(jnp.int32)
    onehot = (block_ids[:, :, None] == jnp.arange(EXPERTS, dtype=jnp.int32)[None, None, :]).astype(jnp.int32)
    slot_ids = lax.optimization_barrier(jnp.sum((jnp.cumsum(onehot, axis=1) - onehot) * onehot, axis=2))
    flat_expert = block_ids.reshape(-1)
    flat_source = jnp.repeat(jnp.arange(sources, dtype=jnp.int32), TOK_DEV * TOP)
    flat_token = jnp.repeat(jnp.arange(TOKENS, dtype=jnp.int32), TOP)
    flat_place = flat_source * CAP + slot_ids.reshape(-1).astype(jnp.int32)
    buffer = jnp.zeros((EXPERTS, sources * CAP, D), tokens.dtype).at[flat_expert, flat_place].set(tokens[flat_token])
    outputs = lax.map(lambda item: expert_ffn(item[0], item[1], item[2], item[3]), (buffer, w_gate, w_up, w_down))
    picked = outputs[flat_expert, flat_place].reshape(TOKENS, TOP, D)
    mixture = lax.optimization_barrier(jnp.sum(picked * gates[:, :, None].astype(jnp.float32), axis=1))
    resid = (tokens.astype(jnp.float32) + mixture).astype(jnp.bfloat16)
    resid_f = resid.astype(jnp.float32)
    squares = lax.optimization_barrier(jnp.mean(resid_f * resid_f, axis=1))
    normed = (resid_f * lax.rsqrt(squares + 1e-06)[:, None] * norm_gain[None, :]).astype(jnp.bfloat16)
    width_block = math.gcd(VOCAB, 8192)
    blocks = VOCAB // width_block
    weight_blocks = lm_weight.reshape(D, blocks, width_block).transpose(1, 0, 2)

    def sweep(carry, item):
        best, mass, chosen = carry
        block_w, index = item
        logits = jnp.dot(normed, block_w, preferred_element_type=jnp.float32)
        new_best = jnp.maximum(best, lax.optimization_barrier(jnp.max(logits, axis=1)))
        mass = mass * jnp.exp(best - new_best) + lax.optimization_barrier(jnp.sum(jnp.exp(logits - new_best[:, None]), axis=1))
        cols = index * width_block + jnp.arange(width_block, dtype=jnp.int32)
        chosen = chosen + lax.optimization_barrier(jnp.sum(jnp.where(cols[None, :] == targets[:, None], logits, 0.0), axis=1))
        return ((new_best, mass, chosen), None)
    start = (jnp.full((TOKENS,), -1e+30, jnp.float32), jnp.zeros((TOKENS,), jnp.float32), jnp.zeros((TOKENS,), jnp.float32))
    (best, mass, chosen), _ = lax.scan(sweep, start, (weight_blocks, jnp.arange(blocks, dtype=jnp.int32)))
    return chosen - best - jnp.log(mass)
```

```python
import jax
import jax.numpy as jnp
from jax import lax
from jax.sharding import PartitionSpec as P

AXES = ("expert", "vocab")
LANES = 128


def swap(value, bit, devices):
    return lax.ppermute(value, AXES, [(d, d ^ (1 << bit)) for d in range(devices)])


def gather_bit(parts, bit, devices):
    got = swap(jnp.concatenate(parts, 0) if len(parts) > 1 else parts[0], bit, devices)
    rows = parts[0].shape[0]
    return parts + [got[i * rows : (i + 1) * rows] for i in range(len(parts))]


def body(tokens, expert_ids, gates, w_gate, w_up, w_down, norm_gain, lm_weight, targets):
    tok_rows, width = tokens.shape
    groups, _, hid = w_gate.shape
    expert_devs = lax.axis_size("expert")
    vocab_devs = lax.axis_size("vocab")
    devices = expert_devs * vocab_devs
    experts_all = groups * expert_devs
    bits = devices.bit_length() - 1
    vocab_bits = vocab_devs.bit_length() - 1
    own = tok_rows // vocab_devs
    half = own // 2
    vocab_index = lax.axis_index("vocab")
    expert_index = lax.axis_index("expert")

    ids_own = lax.dynamic_slice_in_dim(expert_ids, vocab_index * own, own, 0)
    gates_own = lax.dynamic_slice_in_dim(gates, vocab_index * own, own, 0)
    tokens_own = lax.dynamic_slice_in_dim(tokens, vocab_index * own, own, 0)
    targets_own = lax.dynamic_slice_in_dim(targets, vocab_index * own, own, 0)
    every = jnp.arange(experts_all, dtype=jnp.int32)
    coef = jnp.sum(
        jnp.where(ids_own[:, :, None] == every[None, None, :], gates_own[:, :, None], 0.0), axis=1
    )
    coef_hi = coef.astype(jnp.bfloat16)
    coef_lo = (coef - coef_hi.astype(jnp.float32)).astype(jnp.bfloat16)
    digits = jnp.stack(
        [targets_own // 16384, (targets_own // 128) % 128, targets_own % 128], axis=1
    ).astype(jnp.bfloat16)
    used = 2 * experts_all + 3
    extra = -(-used // LANES) * LANES
    payload = jnp.concatenate(
        [tokens_own, coef_hi, coef_lo, digits, jnp.zeros((own, extra - used), jnp.bfloat16)], axis=1
    )

    far = list(range(bits - 1, vocab_bits, -1))
    order = {0: [vocab_bits] + [1], 1: [1] + [vocab_bits]}

    def spread(rows):
        parts = [rows]
        for bit in far:
            parts = gather_bit(parts, bit, devices)
        streams = []
        for stream in (0, 1):
            mine = [p[stream * half : (stream + 1) * half] for p in parts]
            for bit in order[stream]:
                mine = gather_bit(mine, bit, devices)
            streams.append(mine)
        out = []
        for stream in (0, 1):
            near = jnp.concatenate(streams[stream], 0)
            out.append((near, swap(near, 0, devices)))
        return out

    arrived = spread(payload)

    pad = -(-hid // LANES) * LANES - hid
    w_in = jnp.concatenate(
        [jnp.pad(w[l], ((0, 0), (0, pad))) for w in (w_gate, w_up) for l in range(groups)], axis=1
    )
    w_out = jnp.pad(w_down, ((0, 0), (0, pad), (0, 0))).reshape(-1, width)
    wide = groups * (hid + pad)

    def experts(rows):
        both = jnp.dot(rows[:, :width], w_in, preferred_element_type=jnp.float32)
        gate_val, up_val = both[:, :wide], both[:, wide:]
        table = rows[:, width : width + 2 * experts_all].astype(jnp.float32)
        table = table[:, :experts_all] + table[:, experts_all:]
        scale = jnp.concatenate(
            [
                jnp.broadcast_to(
                    jnp.sum(
                        jnp.where(every[None, :] == expert_index * groups + l, table, 0.0),
                        axis=1,
                        keepdims=True,
                    ),
                    (rows.shape[0], hid + pad),
                )
                for l in range(groups)
            ],
            axis=1,
        )
        hidden = (jax.nn.silu(gate_val) * up_val * scale).astype(jnp.bfloat16)
        return jnp.dot(hidden, w_out, preferred_element_type=jnp.float32)

    sums = []
    for stream in (0, 1):
        near, away = arrived[stream]
        sent = swap(experts(away).astype(jnp.bfloat16), 0, devices)
        total = experts(near) + sent.astype(jnp.float32)
        for bit in reversed(order[stream]):
            keep = total.shape[0] // 2
            sent = swap(total[keep:].astype(jnp.bfloat16), bit, devices)
            total = total[:keep] + sent.astype(jnp.float32)
        sums.append(total)
    count = sums[0].shape[0] // half
    total = jnp.concatenate(
        [s[i * half : (i + 1) * half] for i in range(count) for s in sums], axis=0
    )
    for bit in reversed(far):
        keep = total.shape[0] // 2
        sent = swap(total[keep:].astype(jnp.bfloat16), bit, devices)
        total = total[:keep] + sent.astype(jnp.float32)

    resid = (tokens_own.astype(jnp.float32) + total).astype(jnp.bfloat16)
    resid_f = resid.astype(jnp.float32)
    squares = jnp.mean(resid_f * resid_f, axis=1)
    normed = (resid_f * lax.rsqrt(squares + 1e-06)[:, None] * norm_gain[None, :]).astype(
        jnp.bfloat16
    )
    normed_all = spread(normed)

    base = (expert_index * vocab_devs + vocab_index) * lm_weight.shape[1]
    columns = base + jnp.arange(lm_weight.shape[1], dtype=jnp.int32)

    def stats(rows, info):
        place = info[:, width + 2 * experts_all : width + 2 * experts_all + 3].astype(jnp.float32)
        place = (place[:, 0] * 16384 + place[:, 1] * 128 + place[:, 2]).astype(jnp.int32)
        logits = jnp.dot(rows, lm_weight, preferred_element_type=jnp.float32)
        top = jnp.max(logits, axis=1)
        mass = jnp.sum(jnp.exp(logits - top[:, None]), axis=1)
        chosen = jnp.sum(jnp.where(columns[None, :] == place[:, None], logits, 0.0), axis=1)
        return jnp.stack([top, mass, chosen])

    def joined(first, second):
        best = jnp.maximum(first[0], second[0])
        mass = first[1] * jnp.exp(first[0] - best) + second[1] * jnp.exp(second[0] - best)
        return jnp.stack([best, mass, first[2] + second[2]])

    slots = {}
    lows = 1 << len(far)
    for stream in (0, 1):
        for core in (0, 1):
            got = stats(normed_all[stream][core], arrived[stream][core]).reshape(3, -1, half)
            first, second = order[stream]
            for i in range(got.shape[1]):
                slot = core
                for j, bit in enumerate(far):
                    slot |= ((i >> j) & 1) << bit
                slot |= ((i // lows) & 1) << first
                slot |= ((i // lows // 2) & 1) << second
                slots[slot, stream] = got[:, i]
    table = jnp.stack(
        [jnp.concatenate([slots[s, 0], slots[s, 1]], axis=1) for s in range(devices)], axis=1
    )
    for bit in range(vocab_bits):
        flipped = table.reshape(3, devices >> (bit + 1), 2, 1 << bit, own)[:, :, ::-1]
        got = swap(flipped.reshape(3, devices, own), bit, devices)
        table = joined(table, got)
    for bit in range(bits - 1, vocab_bits - 1, -1):
        keep = table.shape[1] // 2
        got = swap(table[:, keep:], bit, devices)
        table = joined(table[:, :keep], got)
    result = table[2] - table[0] - jnp.log(table[1])
    share = jnp.arange(vocab_devs, dtype=jnp.int32)
    ordered = jnp.sum(
        jnp.where(
            (share[:, None] ^ vocab_index == share[None, :])[:, :, None], result[None, :, :], 0.0
        ),
        axis=1,
    )
    return ordered.reshape(tok_rows)


def solution(mesh):
    in_specs = (
        P("expert", None),
        P("expert", None),
        P("expert", None),
        P("expert", None, "vocab"),
        P("expert", None, "vocab"),
        P("expert", "vocab", None),
        P(),
        P(None, ("expert", "vocab")),
        P("expert"),
    )
    return jax.shard_map(
        body, mesh=mesh, in_specs=in_specs, out_specs=P("expert"), check_vma=False
    )
```

```python
import functools

import jax
import jax.numpy as jnp
from jax import lax
from jax.experimental import pallas as pl
from jax.experimental.pallas import tpu as pltpu
from jax.sharding import PartitionSpec as P

AXES = ("expert", "vocab")
LANES = 128


def exchange(value, masks):
    devices = lax.axis_size(AXES)
    return lax.ppermute(value, AXES, [(d, d ^ masks[d & 1]) for d in range(devices)])


def gather_far(own, bits, *early):
    parts = own
    rows = own.shape[0]
    for bit in bits:
        if parts.shape[0] > rows and early:
            parts = lax.optimization_barrier((parts, early))[0]
        pieces = [parts[:rows], parts[rows:]] if parts.shape[0] > rows else [parts]
        parts = jnp.concatenate([parts] + [exchange(p, (1 << bit,) * 2) for p in pieces], axis=0)
    return parts


def reduce_far(total, bits, rows):
    for bit in reversed(bits):
        keep = total.shape[0] // 2
        far = total[keep:].astype(jnp.bfloat16)
        cuts = (keep // 2, 0) if keep > rows else (0,)
        ends = (keep, keep // 2) if keep > rows else (keep,)
        got = [exchange(far[lo:hi], (1 << bit,) * 2).astype(jnp.float32) for lo, hi in zip(cuts, ends)]
        near = [total[lo:hi] + g for lo, hi, g in zip(cuts, ends, got)]
        total = jnp.concatenate(near[::-1], axis=0) if len(near) > 1 else near[0]
    return total


def pack_kernel(place_ref, tokens_ref, ids_ref, gates_ref, targets_ref, out_ref):
    own, total = out_ref.shape
    width = tokens_ref.shape[1]
    first = pl.multiple_of(place_ref[0] * own, own)
    experts_all = place_ref[2]
    out_ref[:, :width] = tokens_ref[pl.ds(first, own)]
    shape = (own, total - width)
    lane = lax.broadcasted_iota(jnp.int32, shape, 1)
    row = lax.broadcasted_iota(jnp.int32, (own, tokens_ref.shape[0]), 0)
    column = lax.broadcasted_iota(jnp.int32, (own, tokens_ref.shape[0]), 1)

    def turned(values):
        return jnp.sum(jnp.where(column == row + first, values, 0.0), axis=1, keepdims=True)

    low = lane >= experts_all
    expert = jnp.where(low, lane - experts_all, lane).astype(jnp.float32)
    coef = jnp.zeros(shape, jnp.float32)
    for k in range(ids_ref.shape[0]):
        chosen = turned(ids_ref[k : k + 1].astype(jnp.float32))
        coef = jnp.where(expert == chosen, turned(gates_ref[k : k + 1]), coef)
    high = coef.astype(jnp.bfloat16).astype(jnp.float32)
    value = jnp.where(low, coef - high, high)
    token = targets_ref[...]
    digits = (token // 16384, (token // 128) % 128, token % 128)
    for j, digit in enumerate(digits):
        value = jnp.where(lane == 2 * experts_all + j, turned(digit.astype(jnp.float32)), value)
    value = jnp.where(lane < 2 * experts_all + len(digits), value, 0.0)
    out_ref[:, width:] = value.astype(jnp.bfloat16)


def packed(place, tokens, expert_ids, gates, targets, own, extra):
    vmem = pl.BlockSpec(memory_space=pltpu.VMEM)
    return pl.pallas_call(
        pack_kernel,
        out_shape=jax.ShapeDtypeStruct((own, tokens.shape[1] + extra), jnp.bfloat16),
        in_specs=[pl.BlockSpec(memory_space=pltpu.SMEM), vmem, vmem, vmem, vmem],
        out_specs=vmem,
        compiler_params=pltpu.CompilerParams(vmem_limit_bytes=4 * 2**20),
        name="pack",
    )(place, tokens, expert_ids, gates, targets)


def load_kernel(order_ref, gate_hbm, up_hbm, down_hbm, gate_out, up_out, down_out, sems):
    groups, hid, _ = gate_hbm.shape
    copies = []
    for m, (src, dst) in enumerate(((gate_hbm, gate_out), (up_hbm, up_out), (down_hbm, down_out))):
        for l in range(groups):
            copy = pltpu.make_async_copy(src.at[l], dst.at[pl.ds(l * hid, hid)], sems.at[m, l])
            copy.start()
            copies.append(copy)
    for copy in copies:
        copy.wait()


def loaded(order, gate_t, up_t, down):
    groups, hid, width = gate_t.shape
    vmem = pl.BlockSpec(memory_space=pltpu.VMEM)
    whole = pl.BlockSpec(memory_space=pltpu.HBM)
    return pl.pallas_call(
        load_kernel,
        out_shape=(jax.ShapeDtypeStruct((groups * hid, width), jnp.bfloat16),) * 3,
        in_specs=[pl.BlockSpec(memory_space=pltpu.SMEM), whole, whole, whole],
        out_specs=(vmem, vmem, vmem),
        scratch_shapes=[pltpu.SemaphoreType.DMA((3, groups))],
        compiler_params=pltpu.CompilerParams(vmem_limit_bytes=12 * 2**20),
        name="load",
    )(order, gate_t, up_t, down)


def expert_kernel(place_ref, near_ref, away_ref, gate_ref, up_ref, down_ref, near_out, away_out,
                  info_out, x_ref, hidden_ref, *, groups):
    units, width = down_ref.shape
    hid = units // groups
    rows = near_ref.shape[0]
    x_ref[:rows] = near_ref[:, :width]
    x_ref[rows:] = away_ref[:, :width]
    info_out[:rows] = near_ref[:, width:]
    info_out[rows:] = away_ref[:, width:]
    table = info_out[...].astype(jnp.float32)
    lane = lax.broadcasted_iota(jnp.int32, table.shape, 1)
    every = place_ref[2]
    unit = lax.broadcasted_iota(jnp.int32, (1, units), 1)
    scale = jnp.zeros((2 * rows, units), jnp.float32)
    for l in range(groups):
        mine = place_ref[1] + l
        hit = (lane == mine) | (lane == mine + every)
        value = jnp.sum(jnp.where(hit, table, 0.0), axis=1, keepdims=True)
        scale = jnp.where((unit >= l * hid) & (unit < (l + 1) * hid), value, scale)
    dims = (((1,), (1,)), ((), ()))
    for lo in range(0, units, 256):
        part = slice(lo, min(lo + 256, units))
        gate_val = lax.dot_general(
            x_ref[...], gate_ref[part], dims, preferred_element_type=jnp.float32
        )
        up_val = lax.dot_general(x_ref[...], up_ref[part], dims, preferred_element_type=jnp.float32)
        hidden = gate_val / (1.0 + jnp.exp(-gate_val)) * up_val * scale[:, part]
        hidden_ref[:, part] = hidden.astype(jnp.bfloat16)
    result = jnp.dot(hidden_ref[...], down_ref[...], preferred_element_type=jnp.float32)
    near_out[...] = result[:rows]
    away_out[...] = result[rows:].astype(jnp.bfloat16)


def experts(place, near, away, matrices, groups):
    units, width = matrices[2].shape
    rows, total = near.shape
    vmem = pl.BlockSpec(memory_space=pltpu.VMEM)
    return pl.pallas_call(
        functools.partial(expert_kernel, groups=groups),
        out_shape=(
            jax.ShapeDtypeStruct((rows, width), jnp.float32),
            jax.ShapeDtypeStruct((rows, width), jnp.bfloat16),
            jax.ShapeDtypeStruct((2 * rows, total - width), jnp.bfloat16),
        ),
        in_specs=[pl.BlockSpec(memory_space=pltpu.SMEM), vmem, vmem, vmem, vmem, vmem],
        out_specs=(vmem, vmem, vmem),
        scratch_shapes=[
            pltpu.VMEM((2 * rows, width), jnp.bfloat16),
            pltpu.VMEM((2 * rows, units), jnp.bfloat16),
        ],
        cost_estimate=pl.CostEstimate(
            flops=12 * rows * units * width, transcendentals=2 * rows * units,
            bytes_accessed=6 * units * width,
        ),
        compiler_params=pltpu.CompilerParams(vmem_limit_bytes=20 * 2**20),
        name="experts",
    )(place, near, away, *matrices)


def stats_kernel(base_ref, near_ref, away_ref, info_ref, weight_ref, out_ref, *, digit):
    rows = near_ref.shape[0]
    weight = weight_ref[...]
    info = info_ref[...].astype(jnp.float32)
    lane = lax.broadcasted_iota(jnp.int32, info.shape, 1)
    place = jnp.zeros((2 * rows, 1), jnp.float32)
    for j, worth in enumerate((16384.0, 128.0, 1.0)):
        place = place + worth * jnp.sum(
            jnp.where(lane == digit + j, info, 0.0), axis=1, keepdims=True
        )
    place = place.astype(jnp.int32) - base_ref[0]
    x = jnp.concatenate([near_ref[...], away_ref[...]], axis=0)
    logits = jnp.dot(x, weight, preferred_element_type=jnp.float32)
    column = lax.broadcasted_iota(jnp.int32, logits.shape, 1)
    top = jnp.max(logits, axis=1, keepdims=True)
    mass = jnp.sum(jnp.exp(logits - top), axis=1, keepdims=True)
    chosen = jnp.sum(jnp.where(column == place, logits, 0.0), axis=1, keepdims=True)
    wide = lax.broadcasted_iota(jnp.int32, (2 * rows, LANES), 1)
    flat = jnp.where(wide == 0, top, jnp.where(wide == 1, mass, chosen))
    out_ref[...] = flat.T[:8]


def row_stats(base, near, away, info, weight, digit):
    rows = near.shape[0]
    vmem = pl.BlockSpec(memory_space=pltpu.VMEM)
    return pl.pallas_call(
        functools.partial(stats_kernel, digit=digit),
        out_shape=jax.ShapeDtypeStruct((8, 2 * rows), jnp.float32),
        in_specs=[pl.BlockSpec(memory_space=pltpu.SMEM), vmem, vmem, vmem, vmem],
        out_specs=vmem,
        cost_estimate=pl.CostEstimate(
            flops=4 * rows * weight.shape[0] * weight.shape[1],
            transcendentals=2 * rows * weight.shape[1], bytes_accessed=2 * weight.size,
        ),
        compiler_params=pltpu.CompilerParams(vmem_limit_bytes=12 * 2**20),
        name="stats",
    )(base, near, away, info, weight)


def body(tokens, expert_ids, gates, w_gate, w_up, w_down, norm_gain, lm_weight, targets):
    tok_rows, width = tokens.shape
    groups, _, hid = w_gate.shape
    expert_devs = lax.axis_size("expert")
    vocab_devs = lax.axis_size("vocab")
    devices = expert_devs * vocab_devs
    experts_all = groups * expert_devs
    bits = devices.bit_length() - 1
    vocab_bits = vocab_devs.bit_length() - 1
    own = tok_rows // vocab_devs
    vocab_index = lax.axis_index("vocab")
    expert_index = lax.axis_index("expert")

    used = 2 * experts_all + 3
    extra = -(-used // LANES) * LANES
    place = jnp.stack([vocab_index, expert_index * groups, experts_all]).astype(jnp.int32)
    payload = packed(place, tokens, expert_ids.T, gates.T, targets.reshape(1, -1), own, extra)
    tokens_own = payload[:, :width]

    far = list(range(bits - 1, vocab_bits, -1))
    step_a = (1 << vocab_bits, 2)
    step_b = (2, 1 << vocab_bits)
    near_swap = (1, 1)

    order = lax.optimization_barrier((place, payload))[0]
    matrices = loaded(order, w_gate.swapaxes(1, 2), w_up.swapaxes(1, 2), w_down)

    def spread(own_rows, work, *early):
        start = gather_far(own_rows, far, *early)
        one = exchange(start, step_a)
        near = (start, exchange(start, near_swap))
        done = [work(near)]
        start, done[0] = lax.optimization_barrier((start, done[0]))
        two = exchange(start, step_b)
        one, done[0] = lax.optimization_barrier((one, done[0]))
        both = exchange(one, step_b)
        done.append(work((one, exchange(one, near_swap))))
        both, done[1] = lax.optimization_barrier((both, done[1]))
        done.append(work((two, exchange(two, near_swap))))
        done.append(work((both, exchange(both, near_swap))))
        return done

    def chip_part(pair):
        return experts(place, pair[0], pair[1], matrices, groups)

    parts = spread(payload, chip_part, *matrices)

    def moved(value, masks):
        return exchange(value.astype(jnp.bfloat16), masks).astype(jnp.float32)

    start, one, two, both = [
        near + exchange(away, near_swap).astype(jnp.float32) for near, away, _ in parts
    ]
    start = start + moved(two, step_b)
    one = one + moved(both, step_b)
    start = start + moved(one, step_a)
    total = reduce_far(start, far, own)

    resid = (tokens_own.astype(jnp.float32) + total).astype(jnp.bfloat16)
    resid_f = resid.astype(jnp.float32)
    squares = jnp.mean(resid_f * resid_f, axis=1)
    normed = (resid_f * lax.rsqrt(squares + 1e-06)[:, None] * norm_gain[None, :]).astype(
        jnp.bfloat16
    )
    base = (expert_index * vocab_devs + vocab_index) * lm_weight.shape[1]
    base = base.reshape(1).astype(jnp.int32)

    def joined(first, second):
        best = jnp.maximum(first[0], second[0])
        mass = first[1] * jnp.exp(first[0] - best) + second[1] * jnp.exp(second[0] - best)
        return jnp.stack([best, mass, first[2] + second[2]])

    infos = iter([part[2] for part in parts])

    def chip_stats(pair):
        return row_stats(base, pair[0], pair[1], next(infos), lm_weight, 2 * experts_all)

    got = [q[:3].reshape(3, 2, -1) for q in spread(normed, chip_stats)]
    table = jnp.stack(got, axis=2).reshape(3, 2, 2, 2, -1)
    odd = vocab_index % 2
    table = jnp.stack(
        [
            jnp.where(odd == 0, table[:, 0], table[:, 0].swapaxes(1, 2)),
            jnp.where(odd == 1, table[:, 1], table[:, 1].swapaxes(1, 2)),
        ],
        axis=1,
    )
    table = joined(table, exchange(table[:, ::-1], near_swap))
    table = joined(table, exchange(table[:, :, ::-1], (2, 2)))
    table = table.reshape(3, 2, 2, 2, 1 << len(far), own).transpose(0, 3, 4, 1, 2, 5)
    table = table.reshape(3, 2 << len(far), 4, own)
    low = 1 << len(far)
    table = joined(table[:, :low], exchange(table[:, low:], (1 << vocab_bits,) * 2))
    for bit in reversed(far):
        low = low // 2
        table = joined(table[:, :low], exchange(table[:, low:], (1 << bit,) * 2))
    result = (table[2] - table[0] - jnp.log(table[1]))[0]
    share = jnp.arange(vocab_devs, dtype=jnp.int32)
    label = (share % 2) * 2 + share // 2
    ordered = jnp.sum(
        jnp.where(
            ((share[:, None] ^ vocab_index) == label[None, :])[:, :, None], result[None, :, :], 0.0
        ),
        axis=1,
    )
    return ordered.reshape(tok_rows)


def solution(mesh):
    in_specs = (
        P("expert", None),
        P("expert", None),
        P("expert", None),
        P("expert", None, "vocab"),
        P("expert", None, "vocab"),
        P("expert", "vocab", None),
        P(),
        P(None, ("expert", "vocab")),
        P("expert"),
    )
    return jax.shard_map(
        body, mesh=mesh, in_specs=in_specs, out_specs=P("expert"), check_vma=False
    )
```

```python
import functools

import jax
import jax.numpy as jnp
from jax import lax
from jax.experimental import pallas as pl
from jax.experimental.pallas import tpu as pltpu
from jax.sharding import PartitionSpec as P


AXES = ("expert", "vocab")
LANES = 128


def chip_bytes(mebibytes, rows):
    return min(56, mebibytes * max(1, rows // 256)) * 2**20


def exchange(value, masks):
    devices = lax.axis_size(AXES)
    return lax.ppermute(value, AXES, [(d, d ^ masks[d & 1]) for d in range(devices)])


def gather_far(own, bits):
    parts = own
    rows = own.shape[0]
    for bit in bits:
        pieces = [parts[:rows], parts[rows:]] if parts.shape[0] > rows else [parts]
        parts = jnp.concatenate([parts] + [exchange(p, (1 << bit,) * 2) for p in pieces], axis=0)
    return parts


def reduce_far(total, bits, rows):
    for bit in reversed(bits):
        keep = total.shape[0] // 2
        far = total[keep:].astype(jnp.bfloat16)
        cuts = (keep // 2, 0) if keep > rows else (0,)
        ends = (keep, keep // 2) if keep > rows else (keep,)
        got = [exchange(far[lo:hi], (1 << bit,) * 2).astype(jnp.float32) for lo, hi in zip(cuts, ends)]
        near = [total[lo:hi] + g for lo, hi, g in zip(cuts, ends, got)]
        total = jnp.concatenate(near[::-1], axis=0) if len(near) > 1 else near[0]
    return total


def pack_kernel(place_ref, tokens_hbm, ids_hbm, gates_hbm, targets_hbm, out_ref,
                tokens_ref, ids_ref, gates_ref, targets_ref, sems):
    own, total = out_ref.shape
    width = tokens_ref.shape[1]
    first = pl.multiple_of(place_ref[0] * own, own)
    experts_all = place_ref[2]
    copies = [
        pltpu.make_async_copy(src, dst, sems.at[i])
        for i, (src, dst) in enumerate((
            (tokens_hbm.at[pl.ds(first, own)], tokens_ref),
            (ids_hbm, ids_ref),
            (gates_hbm, gates_ref),
            (targets_hbm, targets_ref),
        ))
    ]
    for copy in copies:
        copy.start()
    for copy in copies:
        copy.wait()
    out_ref[:, :width] = tokens_ref[...]
    shape = (own, total - width)
    lane = lax.broadcasted_iota(jnp.int32, shape, 1)
    row = lax.broadcasted_iota(jnp.int32, (own, targets_ref.shape[1]), 0)
    column = lax.broadcasted_iota(jnp.int32, (own, targets_ref.shape[1]), 1)

    def turned(values):
        return jnp.sum(jnp.where(column == row + first, values, 0.0), axis=1, keepdims=True)

    low = lane >= experts_all
    expert = jnp.where(low, lane - experts_all, lane).astype(jnp.float32)
    coef = jnp.zeros(shape, jnp.float32)
    for k in range(ids_ref.shape[0]):
        chosen = turned(ids_ref[k : k + 1].astype(jnp.float32))
        coef = jnp.where(expert == chosen, turned(gates_ref[k : k + 1]), coef)
    high = coef.astype(jnp.bfloat16).astype(jnp.float32)
    value = jnp.where(low, coef - high, high)
    token = targets_ref[...]
    digits = (token // 16384, (token // 128) % 128, token % 128)
    for j, digit in enumerate(digits):
        value = jnp.where(lane == 2 * experts_all + j, turned(digit.astype(jnp.float32)), value)
    value = jnp.where(lane < 2 * experts_all + len(digits), value, 0.0)
    out_ref[:, width:] = value.astype(jnp.bfloat16)


def packed(place, tokens, expert_ids, gates, targets, own, extra):
    vmem = pl.BlockSpec(memory_space=pltpu.VMEM)
    return pl.pallas_call(
        pack_kernel,
        out_shape=jax.ShapeDtypeStruct((own, tokens.shape[1] + extra), jnp.bfloat16),
        in_specs=[pl.BlockSpec(memory_space=pltpu.SMEM)] + [pl.BlockSpec(memory_space=pl.ANY)] * 4,
        out_specs=vmem,
        scratch_shapes=[
            pltpu.VMEM((own, tokens.shape[1]), tokens.dtype),
            pltpu.VMEM(expert_ids.shape, expert_ids.dtype),
            pltpu.VMEM(gates.shape, gates.dtype),
            pltpu.VMEM(targets.shape, targets.dtype),
            pltpu.SemaphoreType.DMA((4,)),
        ],
        compiler_params=pltpu.CompilerParams(vmem_limit_bytes=4 * 2**20),
        name="pack",
    )(place, tokens, expert_ids, gates, targets)


def touch_kernel(place_ref, *refs):
    for i in range(place_ref.shape[0]):
        refs[-1][i] = place_ref[i]


def touched(place, matrices):
    vmem = pl.BlockSpec(memory_space=pltpu.VMEM)
    smem = pl.BlockSpec(memory_space=pltpu.SMEM)
    return pl.pallas_call(
        touch_kernel,
        out_shape=jax.ShapeDtypeStruct(place.shape, place.dtype),
        in_specs=[smem] + [vmem] * len(matrices),
        out_specs=smem,
        compiler_params=pltpu.CompilerParams(vmem_limit_bytes=2**20),
        name="touch",
    )(place, *matrices)


def expert_kernel(place_ref, *refs, groups):
    pieces = refs[:-8]
    gate_ref, up_ref, down_ref, near_out, away_out, info_out, x_ref, hidden_ref = refs[-8:]
    units, width = down_ref.shape
    hid = units // groups
    rows = near_out.shape[0]
    piece = pieces[0].shape[0]
    for i, ref in enumerate(pieces):
        x_ref[i * piece : (i + 1) * piece] = ref[:, :width]
        info_out[i * piece : (i + 1) * piece] = ref[:, width:]
    table = info_out[...].astype(jnp.float32)
    lane = lax.broadcasted_iota(jnp.int32, table.shape, 1)
    every = place_ref[2]
    unit = lax.broadcasted_iota(jnp.int32, (1, units), 1)
    scale = jnp.zeros((2 * rows, units), jnp.float32)
    for l in range(groups):
        mine = place_ref[1] + l
        hit = (lane == mine) | (lane == mine + every)
        value = jnp.sum(jnp.where(hit, table, 0.0), axis=1, keepdims=True)
        scale = jnp.where((unit >= l * hid) & (unit < (l + 1) * hid), value, scale)
    dims = (((1,), (1,)), ((), ()))
    for lo in range(0, units, 256):
        part = slice(lo, min(lo + 256, units))
        gate_val = lax.dot_general(
            x_ref[...], gate_ref[part], dims, preferred_element_type=jnp.float32
        )
        up_val = lax.dot_general(x_ref[...], up_ref[part], dims, preferred_element_type=jnp.float32)
        hidden = gate_val / (1.0 + jnp.exp(-gate_val)) * up_val * scale[:, part]
        hidden_ref[:, part] = hidden.astype(jnp.bfloat16)
    result = jnp.dot(hidden_ref[...], down_ref[...], preferred_element_type=jnp.float32)
    near_out[...] = result[:rows]
    away_out[...] = result[rows:].astype(jnp.bfloat16)


def experts(place, pieces, matrices, groups):
    units, width = matrices[2].shape
    rows, total = len(pieces) // 2 * pieces[0].shape[0], pieces[0].shape[1]
    vmem = pl.BlockSpec(memory_space=pltpu.VMEM)
    return pl.pallas_call(
        functools.partial(expert_kernel, groups=groups),
        out_shape=(
            jax.ShapeDtypeStruct((rows, width), jnp.float32),
            jax.ShapeDtypeStruct((rows, width), jnp.bfloat16),
            jax.ShapeDtypeStruct((2 * rows, total - width), jnp.bfloat16),
        ),
        in_specs=[pl.BlockSpec(memory_space=pltpu.SMEM)] + [vmem] * (len(pieces) + 3),
        out_specs=(vmem, vmem, vmem),
        scratch_shapes=[
            pltpu.VMEM((2 * rows, width), jnp.bfloat16),
            pltpu.VMEM((2 * rows, units), jnp.bfloat16),
        ],
        cost_estimate=pl.CostEstimate(
            flops=12 * rows * units * width, transcendentals=2 * rows * units,
            bytes_accessed=6 * units * width,
        ),
        compiler_params=pltpu.CompilerParams(vmem_limit_bytes=chip_bytes(20, 2 * rows)),
        name="experts",
    )(place, *pieces, *matrices)


def stats_kernel(base_ref, *refs, digit):
    pieces = refs[:-3]
    info_ref, weight_ref, out_ref = refs[-3:]
    rows = out_ref.shape[1]
    weight = weight_ref[...]
    info = info_ref[...].astype(jnp.float32)
    lane = lax.broadcasted_iota(jnp.int32, info.shape, 1)
    place = jnp.zeros((rows, 1), jnp.float32)
    for j, worth in enumerate((16384.0, 128.0, 1.0)):
        place = place + worth * jnp.sum(
            jnp.where(lane == digit + j, info, 0.0), axis=1, keepdims=True
        )
    place = place.astype(jnp.int32) - base_ref[0]
    x = jnp.concatenate([ref[...] for ref in pieces], axis=0)
    logits = jnp.dot(x, weight, preferred_element_type=jnp.float32)
    column = lax.broadcasted_iota(jnp.int32, logits.shape, 1)
    top = jnp.max(logits, axis=1, keepdims=True)
    mass = jnp.sum(jnp.exp(logits - top), axis=1, keepdims=True)
    chosen = jnp.sum(jnp.where(column == place, logits, 0.0), axis=1, keepdims=True)
    wide = lax.broadcasted_iota(jnp.int32, (rows, LANES), 1)
    flat = jnp.where(wide == 0, top, jnp.where(wide == 1, mass, chosen))
    out_ref[...] = flat.T[:8]


def row_stats(base, pieces, info, weight, digit):
    rows = len(pieces) * pieces[0].shape[0]
    vmem = pl.BlockSpec(memory_space=pltpu.VMEM)
    return pl.pallas_call(
        functools.partial(stats_kernel, digit=digit),
        out_shape=jax.ShapeDtypeStruct((8, rows), jnp.float32),
        in_specs=[pl.BlockSpec(memory_space=pltpu.SMEM)] + [vmem] * (len(pieces) + 2),
        out_specs=vmem,
        cost_estimate=pl.CostEstimate(
            flops=2 * rows * weight.shape[0] * weight.shape[1],
            transcendentals=rows * weight.shape[1], bytes_accessed=2 * weight.size,
        ),
        compiler_params=pltpu.CompilerParams(vmem_limit_bytes=chip_bytes(12, rows)),
        name="stats",
    )(base, *pieces, info, weight)


def layer(tokens, expert_ids, gates, w_gate, w_up, w_down, norm_gain, lm_weight, targets):
    tok_rows, width = tokens.shape
    groups, _, hid = w_gate.shape
    expert_devs = lax.axis_size("expert")
    vocab_devs = lax.axis_size("vocab")
    devices = expert_devs * vocab_devs
    experts_all = groups * expert_devs
    bits = devices.bit_length() - 1
    vocab_bits = vocab_devs.bit_length() - 1
    own = tok_rows // vocab_devs
    vocab_index = lax.axis_index("vocab")
    expert_index = lax.axis_index("expert")

    used = 2 * experts_all + 3
    extra = -(-used // LANES) * LANES
    place = jnp.stack([vocab_index, expert_index * groups, experts_all]).astype(jnp.int32)
    payload = packed(place, tokens, expert_ids.T, gates.T, targets.reshape(1, -1), own, extra)
    tokens_own = payload[:, :width]

    far = list(range(bits - 1, vocab_bits, -1))
    step_a = (1 << vocab_bits, 2)
    step_b = (2, 1 << vocab_bits)
    near_swap = (1, 1)

    units = groups * hid
    matrices = (
        w_gate.swapaxes(1, 2).reshape(units, width),
        w_up.swapaxes(1, 2).reshape(units, width),
        w_down.reshape(units, width),
    )
    last = (1 << far[-1],) * 2

    def crossed(value):
        return exchange(value, near_swap)

    def spread(own_rows, work):
        early = gather_far(own_rows, far[:-1])[own:]
        middle = exchange(own_rows, last)
        final = exchange(early, last)
        done = []
        for g, start in enumerate((own_rows, jnp.concatenate([early, middle], 0), final)):
            one = exchange(start, step_a)
            two = exchange(start, step_b)
            both = exchange(one, step_b)
            calls = ((start, one), (two, both)) if g == 1 else ((start, one, two, both),)
            for near in calls:
                pieces = near + tuple(crossed(p) for p in near)
                done.append(work(pieces))
        return done

    def moved(value, masks):
        return exchange(value.astype(jnp.bfloat16), masks).astype(jnp.float32)

    def chip_part(pieces):
        return experts(place, pieces, matrices, groups)

    place = touched(touched(place, matrices[:2]), matrices[2:])
    parts = spread(payload, chip_part)
    totals = []
    for calls in (parts[:1], parts[1:3], parts[3:]):
        kept = [near + crossed(away).astype(jnp.float32) for near, away, _ in calls]
        size = kept[0].shape[0] * len(calls) // 4
        start, one, two, both = [k[i : i + size] for k in kept for i in range(0, len(k), size)]
        one = one + moved(both, step_b)
        start = start + moved(two, step_b)
        totals.append(start + moved(one, step_a))
    rest = totals[1][:-own] + moved(totals[2], last)
    total = totals[0] + moved(totals[1][-own:], last)
    if len(far) == 2:
        total = total + moved(rest, (1 << far[0],) * 2)
    else:
        total = reduce_far(jnp.concatenate([total, rest], 0), far[:-1], own)

    resid = (tokens_own.astype(jnp.float32) + total).astype(jnp.bfloat16)
    resid_f = resid.astype(jnp.float32)
    squares = jnp.mean(resid_f * resid_f, axis=1)
    normed = (resid_f * lax.rsqrt(squares + 1e-06)[:, None] * norm_gain[None, :]).astype(
        jnp.bfloat16
    )
    base = (expert_index * vocab_devs + vocab_index) * lm_weight.shape[1]
    base = base.reshape(1).astype(jnp.int32)

    def joined(first, second):
        best = jnp.maximum(first[0], second[0])
        mass = first[1] * jnp.exp(first[0] - best) + second[1] * jnp.exp(second[0] - best)
        return jnp.stack([best, mass, first[2] + second[2]])

    infos = iter([part[2] for part in parts])

    def chip_stats(pieces):
        return row_stats(base, pieces, next(infos), lm_weight, 2 * experts_all)

    got = [q[:3] for q in spread(normed, chip_stats)]
    table = jnp.concatenate(
        [
            got[0].reshape(3, 2, 2, 2, -1),
            jnp.stack([q.reshape(3, 2, 2, -1) for q in got[1:3]], axis=2),
            got[3].reshape(3, 2, 2, 2, -1),
        ],
        axis=4,
    )
    odd = vocab_index % 2
    table = jnp.stack(
        [
            jnp.where(odd == 0, table[:, 0], table[:, 0].swapaxes(1, 2)),
            jnp.where(odd == 1, table[:, 1], table[:, 1].swapaxes(1, 2)),
        ],
        axis=1,
    )
    table = joined(table, exchange(table[:, ::-1], near_swap))
    table = joined(table, exchange(table[:, :, ::-1], (2, 2)))
    table = table.reshape(3, 2, 2, 2, 1 << len(far), own).transpose(0, 3, 4, 1, 2, 5)
    table = table.reshape(3, 2 << len(far), 4, own)
    low = 1 << len(far)
    table = joined(table[:, :low], exchange(table[:, low:], (1 << vocab_bits,) * 2))
    for bit in reversed(far):
        low = low // 2
        table = joined(table[:, :low], exchange(table[:, low:], (1 << bit,) * 2))
    result = (table[2] - table[0] - jnp.log(table[1]))[0]
    share = jnp.arange(vocab_devs, dtype=jnp.int32)
    label = (share % 2) * 2 + share // 2
    ordered = jnp.sum(
        jnp.where(
            ((share[:, None] ^ vocab_index) == label[None, :])[:, :, None], result[None, :, :], 0.0
        ),
        axis=1,
    )
    return ordered.reshape(tok_rows)


def solution(mesh):
    in_specs = (
        P("expert", None),
        P("expert", None),
        P("expert", None),
        P("expert", None, "vocab"),
        P("expert", None, "vocab"),
        P("expert", "vocab", None),
        P(),
        P(None, ("expert", "vocab")),
        P("expert"),
    )
    return jax.shard_map(
        layer, mesh=mesh, in_specs=in_specs, out_specs=P("expert"), check_vma=False
    )
```

```python
import functools

import jax
import jax.numpy as jnp
from jax import lax
from jax.experimental import pallas as pl
from jax.experimental.pallas import tpu as pltpu
from jax.sharding import PartitionSpec as P


AXES = ("expert", "vocab")
LANES = 128


def chip_bytes(mebibytes, rows):
    return min(56, mebibytes * max(1, rows // 256)) * 2**20


def exchange(value, masks):
    devices = lax.axis_size(AXES)
    return lax.ppermute(value, AXES, [(d, d ^ masks[d & 1]) for d in range(devices)])


def gather_far(own, bits):
    parts = own
    rows = own.shape[0]
    for bit in bits:
        pieces = [parts[:rows], parts[rows:]] if parts.shape[0] > rows else [parts]
        parts = jnp.concatenate([parts] + [exchange(p, (1 << bit,) * 2) for p in pieces], axis=0)
    return parts


def reduce_far(total, bits, rows):
    for bit in reversed(bits):
        keep = total.shape[0] // 2
        far = total[keep:].astype(jnp.bfloat16)
        cuts = (keep // 2, 0) if keep > rows else (0,)
        ends = (keep, keep // 2) if keep > rows else (keep,)
        got = [exchange(far[lo:hi], (1 << bit,) * 2).astype(jnp.float32) for lo, hi in zip(cuts, ends)]
        near = [total[lo:hi] + g for lo, hi, g in zip(cuts, ends, got)]
        total = jnp.concatenate(near[::-1], axis=0) if len(near) > 1 else near[0]
    return total


def pack_kernel(place_ref, tokens_hbm, ids_hbm, gates_hbm, targets_hbm, out_ref,
                tokens_ref, ids_ref, gates_ref, targets_ref, sems):
    own, total = out_ref.shape
    width = tokens_ref.shape[1]
    first = pl.multiple_of(place_ref[0] * own, own)
    experts_all = place_ref[2]
    copies = [
        pltpu.make_async_copy(src, dst, sems.at[i])
        for i, (src, dst) in enumerate((
            (tokens_hbm.at[pl.ds(first, own)], tokens_ref),
            (ids_hbm, ids_ref),
            (gates_hbm, gates_ref),
            (targets_hbm, targets_ref),
        ))
    ]
    for copy in copies:
        copy.start()
    for copy in copies:
        copy.wait()
    out_ref[:, :width] = tokens_ref[...]
    shape = (own, total - width)
    lane = lax.broadcasted_iota(jnp.int32, shape, 1)
    row = lax.broadcasted_iota(jnp.int32, (own, targets_ref.shape[1]), 0)
    column = lax.broadcasted_iota(jnp.int32, (own, targets_ref.shape[1]), 1)

    def turned(values):
        return jnp.sum(jnp.where(column == row + first, values, 0.0), axis=1, keepdims=True)

    low = lane >= experts_all
    expert = jnp.where(low, lane - experts_all, lane).astype(jnp.float32)
    coef = jnp.zeros(shape, jnp.float32)
    for k in range(ids_ref.shape[0]):
        chosen = turned(ids_ref[k : k + 1].astype(jnp.float32))
        coef = jnp.where(expert == chosen, turned(gates_ref[k : k + 1]), coef)
    high = coef.astype(jnp.bfloat16).astype(jnp.float32)
    value = jnp.where(low, coef - high, high)
    token = targets_ref[...]
    digits = (token // 16384, (token // 128) % 128, token % 128)
    for j, digit in enumerate(digits):
        value = jnp.where(lane == 2 * experts_all + j, turned(digit.astype(jnp.float32)), value)
    value = jnp.where(lane < 2 * experts_all + len(digits), value, 0.0)
    out_ref[:, width:] = value.astype(jnp.bfloat16)


def packed(place, tokens, expert_ids, gates, targets, own, extra):
    vmem = pl.BlockSpec(memory_space=pltpu.VMEM)
    return pl.pallas_call(
        pack_kernel,
        out_shape=jax.ShapeDtypeStruct((own, tokens.shape[1] + extra), jnp.bfloat16),
        in_specs=[pl.BlockSpec(memory_space=pltpu.SMEM)] + [pl.BlockSpec(memory_space=pl.ANY)] * 4,
        out_specs=vmem,
        scratch_shapes=[
            pltpu.VMEM((own, tokens.shape[1]), tokens.dtype),
            pltpu.VMEM(expert_ids.shape, expert_ids.dtype),
            pltpu.VMEM(gates.shape, gates.dtype),
            pltpu.VMEM(targets.shape, targets.dtype),
            pltpu.SemaphoreType.DMA((4,)),
        ],
        compiler_params=pltpu.CompilerParams(vmem_limit_bytes=4 * 2**20),
        name="pack",
    )(place, tokens, expert_ids, gates, targets)


def touch_kernel(matrix_ref, out_ref):
    out_ref[...] = jnp.zeros(out_ref.shape, out_ref.dtype)


def touched(matrix):
    vmem = pl.BlockSpec(memory_space=pltpu.VMEM)
    return pl.pallas_call(
        touch_kernel,
        out_shape=jax.ShapeDtypeStruct((8, LANES), jnp.float32),
        in_specs=[vmem],
        out_specs=vmem,
        compiler_params=pltpu.CompilerParams(vmem_limit_bytes=2**20),
        name="touch",
    )(matrix)


def expert_kernel(place_ref, *refs, groups):
    pieces = refs[:-11]
    gate_ref, up_ref, down_ref, near_out, away_out, info_out, x_ref, hidden_ref = refs[-8:]
    units, width = down_ref.shape
    hid = units // groups
    rows = near_out.shape[0]
    piece = pieces[0].shape[0]
    for i, ref in enumerate(pieces):
        x_ref[i * piece : (i + 1) * piece] = ref[:, :width]
        info_out[i * piece : (i + 1) * piece] = ref[:, width:]
    table = info_out[...].astype(jnp.float32)
    lane = lax.broadcasted_iota(jnp.int32, table.shape, 1)
    every = place_ref[2]
    unit = lax.broadcasted_iota(jnp.int32, (1, units), 1)
    scale = jnp.zeros((2 * rows, units), jnp.float32)
    for l in range(groups):
        mine = place_ref[1] + l
        hit = (lane == mine) | (lane == mine + every)
        value = jnp.sum(jnp.where(hit, table, 0.0), axis=1, keepdims=True)
        scale = jnp.where((unit >= l * hid) & (unit < (l + 1) * hid), value, scale)
    dims = (((1,), (1,)), ((), ()))
    for lo in range(0, units, 256):
        part = slice(lo, min(lo + 256, units))
        gate_val = lax.dot_general(
            x_ref[...], gate_ref[part], dims, preferred_element_type=jnp.float32
        )
        up_val = lax.dot_general(x_ref[...], up_ref[part], dims, preferred_element_type=jnp.float32)
        hidden = gate_val / (1.0 + jnp.exp(-gate_val)) * up_val * scale[:, part]
        hidden_ref[:, part] = hidden.astype(jnp.bfloat16)
    result = jnp.dot(hidden_ref[...], down_ref[...], preferred_element_type=jnp.float32)
    near_out[...] = result[:rows]
    away_out[...] = result[rows:].astype(jnp.bfloat16)


def experts(place, pieces, seen, matrices, groups):
    units, width = matrices[2].shape
    rows, total = len(pieces) // 2 * pieces[0].shape[0], pieces[0].shape[1]
    vmem = pl.BlockSpec(memory_space=pltpu.VMEM)
    return pl.pallas_call(
        functools.partial(expert_kernel, groups=groups),
        out_shape=(
            jax.ShapeDtypeStruct((rows, width), jnp.float32),
            jax.ShapeDtypeStruct((rows, width), jnp.bfloat16),
            jax.ShapeDtypeStruct((2 * rows, total - width), jnp.bfloat16),
        ),
        in_specs=[pl.BlockSpec(memory_space=pltpu.SMEM)] + [vmem] * (len(pieces) + 6),
        out_specs=(vmem, vmem, vmem),
        scratch_shapes=[
            pltpu.VMEM((2 * rows, width), jnp.bfloat16),
            pltpu.VMEM((2 * rows, units), jnp.bfloat16),
        ],
        cost_estimate=pl.CostEstimate(
            flops=12 * rows * units * width, transcendentals=2 * rows * units,
            bytes_accessed=6 * units * width,
        ),
        compiler_params=pltpu.CompilerParams(vmem_limit_bytes=chip_bytes(20, 2 * rows)),
        name="experts",
    )(place, *pieces, *seen, *matrices)


def stats_kernel(place_ref, *refs, digit):
    pieces = refs[:-3]
    info_ref, weight_ref, out_ref = refs[-3:]
    rows = out_ref.shape[1]
    weight = weight_ref[...]
    info = info_ref[...].astype(jnp.float32)
    lane = lax.broadcasted_iota(jnp.int32, info.shape, 1)
    place = jnp.zeros((rows, 1), jnp.float32)
    for j, worth in enumerate((16384.0, 128.0, 1.0)):
        place = place + worth * jnp.sum(
            jnp.where(lane == digit + j, info, 0.0), axis=1, keepdims=True
        )
    place = place.astype(jnp.int32) - place_ref[3]
    x = jnp.concatenate([ref[...] for ref in pieces], axis=0)
    logits = jnp.dot(x, weight, preferred_element_type=jnp.float32)
    column = lax.broadcasted_iota(jnp.int32, logits.shape, 1)
    top = jnp.max(logits, axis=1, keepdims=True)
    mass = jnp.sum(jnp.exp(logits - top), axis=1, keepdims=True)
    chosen = jnp.sum(jnp.where(column == place, logits, 0.0), axis=1, keepdims=True)
    wide = lax.broadcasted_iota(jnp.int32, (rows, LANES), 1)
    flat = jnp.where(wide == 0, top, jnp.where(wide == 1, mass, chosen))
    out_ref[...] = flat.T[:8]


def row_stats(where, pieces, info, weight, digit):
    rows = len(pieces) * pieces[0].shape[0]
    vmem = pl.BlockSpec(memory_space=pltpu.VMEM)
    return pl.pallas_call(
        functools.partial(stats_kernel, digit=digit),
        out_shape=jax.ShapeDtypeStruct((8, rows), jnp.float32),
        in_specs=[pl.BlockSpec(memory_space=pltpu.SMEM)] + [vmem] * (len(pieces) + 2),
        out_specs=vmem,
        cost_estimate=pl.CostEstimate(
            flops=2 * rows * weight.shape[0] * weight.shape[1],
            transcendentals=rows * weight.shape[1], bytes_accessed=2 * weight.size,
        ),
        compiler_params=pltpu.CompilerParams(vmem_limit_bytes=chip_bytes(12, rows)),
        name="stats",
    )(where, *pieces, info, weight)


def layer(tokens, expert_ids, gates, w_gate, w_up, w_down, norm_gain, lm_weight, targets):
    tok_rows, width = tokens.shape
    groups, _, hid = w_gate.shape
    expert_devs = lax.axis_size("expert")
    vocab_devs = lax.axis_size("vocab")
    devices = expert_devs * vocab_devs
    experts_all = groups * expert_devs
    bits = devices.bit_length() - 1
    vocab_bits = vocab_devs.bit_length() - 1
    own = tok_rows // vocab_devs
    vocab_index = lax.axis_index("vocab")
    expert_index = lax.axis_index("expert")

    used = 2 * experts_all + 3
    extra = -(-used // LANES) * LANES
    base = (expert_index * vocab_devs + vocab_index) * lm_weight.shape[1]
    place = jnp.stack([vocab_index, expert_index * groups, experts_all, base]).astype(jnp.int32)
    payload = packed(place, tokens, expert_ids.T, gates.T, targets.reshape(1, -1), own, extra)
    tokens_own = payload[:, :width]

    far = list(range(bits - 1, vocab_bits, -1))
    step_a = (1 << vocab_bits, 2)
    step_b = (2, 1 << vocab_bits)
    near_swap = (1, 1)

    units = groups * hid
    matrices = (
        w_gate.swapaxes(1, 2).reshape(units, width),
        w_up.swapaxes(1, 2).reshape(units, width),
        w_down.reshape(units, width),
    )
    last = (1 << far[-1],) * 2

    def crossed(value):
        return exchange(value, near_swap)

    def spread(own_rows, work):
        early = gather_far(own_rows, far[:-1])[own:]
        middle = exchange(own_rows, last)
        final = exchange(early, last)
        done = []
        for g, start in enumerate((own_rows, jnp.concatenate([early, middle], 0), final)):
            one = exchange(start, step_a)
            two = exchange(start, step_b)
            both = exchange(one, step_b)
            calls = ((start, one), (two, both)) if g == 1 else ((start, one, two, both),)
            for near in calls:
                pieces = near + tuple(crossed(p) for p in near)
                done.append(work(pieces))
        return done

    def moved(value, masks):
        return exchange(value.astype(jnp.bfloat16), masks).astype(jnp.float32)

    def chip_part(pieces):
        return experts(place, pieces, seen, matrices, groups)

    seen = [touched(matrix) for matrix in matrices]
    parts = spread(payload, chip_part)
    totals = []
    for calls in (parts[:1], parts[1:3], parts[3:]):
        kept = [near + crossed(away).astype(jnp.float32) for near, away, _ in calls]
        size = kept[0].shape[0] * len(calls) // 4
        start, one, two, both = [k[i : i + size] for k in kept for i in range(0, len(k), size)]
        one = one + moved(both, step_b)
        start = start + moved(two, step_b)
        totals.append(start + moved(one, step_a))
    rest = totals[1][:-own] + moved(totals[2], last)
    total = totals[0] + moved(totals[1][-own:], last)
    if len(far) == 2:
        total = total + moved(rest, (1 << far[0],) * 2)
    else:
        total = reduce_far(jnp.concatenate([total, rest], 0), far[:-1], own)

    resid = (tokens_own.astype(jnp.float32) + total).astype(jnp.bfloat16)
    resid_f = resid.astype(jnp.float32)
    squares = jnp.mean(resid_f * resid_f, axis=1)
    normed = (resid_f * lax.rsqrt(squares + 1e-06)[:, None] * norm_gain[None, :]).astype(
        jnp.bfloat16
    )

    def joined(first, second):
        best = jnp.maximum(first[0], second[0])
        mass = first[1] * jnp.exp(first[0] - best) + second[1] * jnp.exp(second[0] - best)
        return jnp.stack([best, mass, first[2] + second[2]])

    infos = iter([part[2] for part in parts])

    def chip_stats(pieces):
        return row_stats(place, pieces, next(infos), lm_weight, 2 * experts_all)

    got = spread(normed, chip_stats)
    got, vocab_index = lax.optimization_barrier((got, vocab_index))
    got = [q[:3] for q in got]
    table = jnp.concatenate(
        [
            got[0].reshape(3, 2, 2, 2, -1),
            jnp.stack([q.reshape(3, 2, 2, -1) for q in got[1:3]], axis=2),
            got[3].reshape(3, 2, 2, 2, -1),
        ],
        axis=4,
    )
    odd = vocab_index % 2
    table = jnp.stack(
        [
            jnp.where(odd == 0, table[:, 0], table[:, 0].swapaxes(1, 2)),
            jnp.where(odd == 1, table[:, 1], table[:, 1].swapaxes(1, 2)),
        ],
        axis=1,
    )
    table = joined(table, exchange(table[:, ::-1], near_swap))
    table = joined(table, exchange(table[:, :, ::-1], (2, 2)))
    table = table.reshape(3, 2, 2, 2, 1 << len(far), own).transpose(0, 3, 4, 1, 2, 5)
    table = table.reshape(3, 2 << len(far), 4, own)
    low = 1 << len(far)
    table = joined(table[:, :low], exchange(table[:, low:], (1 << vocab_bits,) * 2))
    for bit in reversed(far):
        low = low // 2
        table = joined(table[:, :low], exchange(table[:, low:], (1 << bit,) * 2))
    result = (table[2] - table[0] - jnp.log(table[1]))[0]
    share = jnp.arange(vocab_devs, dtype=jnp.int32)
    label = (share % 2) * 2 + share // 2
    ordered = jnp.sum(
        jnp.where(
            ((share[:, None] ^ vocab_index) == label[None, :])[:, :, None], result[None, :, :], 0.0
        ),
        axis=1,
    )
    return ordered.reshape(tok_rows)


def solution(mesh):
    in_specs = (
        P("expert", None),
        P("expert", None),
        P("expert", None),
        P("expert", None, "vocab"),
        P("expert", None, "vocab"),
        P("expert", "vocab", None),
        P(),
        P(None, ("expert", "vocab")),
        P("expert"),
    )
    return jax.shard_map(
        layer, mesh=mesh, in_specs=in_specs, out_specs=P("expert"), check_vma=False
    )
```
